128 devices in a mesh: cp: 4 (over x), dp: 32 (over z, y, core).
Axes of the slice: x: 4, y: 4, z: 4, core: 2. Of those that a mesh axis runs over, the one named last changes fastest.
Arguments:
- tokens: bfloat16 [32, 1536, 7168], P('dp', 'cp')
- choices: int32 [32, 1536, 8], P('dp', 'cp')
- router_w: float32 [256, 7168], replicated
- expert_bias: float32 [256], replicated
Outputs:
- output 1: float32 [], replicated
- output 2: float32 [256, 7168], replicated
- output 3: bfloat16 [32, 1536, 7168], P('dp', 'cp')
- output 4: float32 [256], replicated
All inputs are finite; a program needn't handle non-finite values.
Results may differ from the reference program's by a relative error of at most 0.001.
Values sent between devices are 32-bit elements.
A program may use at most 1 GiB of HBM per device.

```python
import jax
import jax.numpy as jnp
from jax import lax

ROWS = 32
SEQ = 1536
EXPERTS = 256
TOP = 8
DIM = 7168
ALPHA = 0.1
GAMMA = 0.001


def draw_choices(route_key, glob_key, seq_key):
    noise = jax.random.randint(route_key, (ROWS, SEQ, EXPERTS), 0, 1024)
    glob_pref = jax.random.randint(glob_key, (EXPERTS,), 0, 768)
    seq_pref = jax.random.randint(seq_key, (ROWS, 1, EXPERTS), 0, 512)
    score = (noise + glob_pref + seq_pref) * EXPERTS + jnp.arange(EXPERTS, dtype=jnp.int32)
    return lax.top_k(score, TOP)[1].astype(jnp.int32)


def setup_inputs(seed: int = 0) -> dict:
    root_key = jax.random.key(seed)
    tok_key, route_key, glob_key, seq_key, gate_key, bias_key = jax.random.split(root_key, 6)
    tokens = jax.random.normal(tok_key, (ROWS, SEQ, DIM), jnp.float32).astype(jnp.bfloat16)
    choices = draw_choices(route_key, glob_key, seq_key)
    router_w = jax.random.normal(gate_key, (EXPERTS, DIM), jnp.float32) * (DIM ** -0.5)
    expert_bias = jax.random.normal(bias_key, (EXPERTS,), jnp.float32) * GAMMA
    return {"tokens": tokens, "choices": choices, "router_w": router_w, "expert_bias": expert_bias}


def reference(tokens, choices, router_w, expert_bias):
    expert_ids = jnp.arange(EXPERTS, dtype=jnp.int32)

    def seq_step(carry, row):
        row_tok, row_choice = row
        counts = jnp.sum((row_choice[:, :, None] == expert_ids).astype(jnp.float32), axis=(0, 1))
        load_frac = counts * (EXPERTS / (TOP * SEQ))

        def seq_loss(weights, toks):
            logits = jnp.dot(toks, weights.T, preferred_element_type=jnp.float32)
            sig_probs = jax.nn.sigmoid(logits)
            normed = sig_probs / jnp.sum(sig_probs, axis=-1, keepdims=True)
            mean_prob = jnp.mean(normed, axis=0)
            return jnp.sum(load_frac * mean_prob) * (ALPHA / ROWS)

        loss_val, pull_back = jax.vjp(seq_loss, router_w, row_tok.astype(jnp.float32))
        grad_w, grad_x = pull_back(jnp.ones_like(loss_val))
        new_carry = (carry[0] + grad_w, carry[1] + loss_val)
        return new_carry, (grad_x.astype(jnp.bfloat16), counts)

    init = (jnp.zeros((EXPERTS, DIM), jnp.float32), jnp.zeros((), jnp.float32))
    (grad_router, bal_loss), (grad_tokens, counts) = lax.scan(seq_step, init, (tokens, choices))
    global_load = jnp.sum(counts, axis=0)
    load_gap = ROWS * SEQ * TOP - EXPERTS * global_load.astype(jnp.int32)
    new_bias = expert_bias + GAMMA * jnp.sign(load_gap).astype(jnp.float32)
    return bal_loss, grad_router, grad_tokens, new_bias
```

```python
import functools

import jax
import jax.numpy as jnp
from jax import lax
from jax.experimental import pallas as pl
from jax.experimental.pallas import tpu as pltpu
from jax.sharding import PartitionSpec as P

ALPHA = 0.1
GAMMA = 0.001
MESH = pl.DeviceIdType.MESH
LANES = 128
RING = 4
STEPS = (1, RING - 1)
UNIT = 256
DX_COLS = 512
LOAD_COLS = 1024
CHUNKS = 2


def split3(v):
    a = v.astype(jnp.bfloat16)
    r = v - a.astype(jnp.float32)
    b = r.astype(jnp.bfloat16)
    c = (r - b.astype(jnp.float32)).astype(jnp.bfloat16)
    return a, b, c


def dot_nt(a, b):
    return lax.dot_general(a, b, (((1,), (1,)), ((), ())), preferred_element_type=jnp.float32)


def dot_nn(a, b):
    return lax.dot_general(a, b, (((1,), (0,)), ((), ())), preferred_element_type=jnp.float32)


def make_regions(dim):
    tiles = dim // LANES
    num = CHUNKS * 3
    base, extra = divmod(tiles, num)
    widths = [base] * num
    for i in range(extra):
        widths[i * 4 % num if num > 4 else i] += 1
    out, at = [], 0
    for q, wd in enumerate(widths):
        half = (wd + 1) // 2
        out.append((q // 3, q % 3, at * LANES, wd * LANES, half * LANES))
        at += wd
    return out


def kernel(sizes, x_hbm, c_hbm, w_hbm, bias_ref, dw, dx, stat_ref, xv, cv, ws, part, acc, r1, r2, r3, zs, gs, gts, sbuf, srecv,
           load_sem, send_sem, recv_sem):
    experts, dim, toks, choice_num, rows_all, seq_all = sizes
    half_e = experts // 2
    p1 = half_e // RING
    p2 = p1 // RING
    cp = lax.axis_index("cp")
    dp = lax.axis_index("dp")
    core = lax.rem(dp, 2)
    y = lax.rem(dp // 2, RING)
    zc = dp // (2 * RING)
    coord = (cp, y, zc)
    other = 1 - core

    def peer(axis, step):
        if axis == 3:
            return (cp, dp + 1 - 2 * core)
        moved = lax.rem(coord[axis] + step, RING)
        if axis == 0:
            return (moved, dp)
        if axis == 1:
            return (cp, zc * (2 * RING) + moved * 2 + core)
        return (cp, moved * (2 * RING) + y * 2 + core)

    copies = {}
    count = [0]

    def send(key, src, dst, to):
        i = count[0]
        count[0] += 1
        cpy = pltpu.make_async_remote_copy(src_ref=src, dst_ref=dst, send_sem=send_sem.at[i], recv_sem=recv_sem.at[i],
                                           device_id=to, device_id_type=MESH)
        cpy.start()
        copies[key] = cpy

    def arrive(key):
        copies[key].wait_recv()

    nload = dim // LOAD_COLS

    def load(j):
        cols = pl.ds(pl.multiple_of(j * LOAD_COLS, LOAD_COLS), LOAD_COLS)
        return (pltpu.make_async_copy(x_hbm.at[:, cols], xv.at[:, cols], load_sem.at[j]),
                pltpu.make_async_copy(w_hbm.at[:, cols], part.at[:, cols], load_sem.at[nload + j]))

    c_copy = pltpu.make_async_copy(c_hbm, cv, load_sem.at[2 * nload])
    c_copy.start()

    @pl.loop(0, nload)
    def _(j):
        a, b = load(j)
        b.start()
        a.start()

    barrier = pltpu.get_barrier_semaphore()
    for axis in range(3):
        for step in (1, 2, 3):
            pl.semaphore_signal(barrier, inc=1, device_id=peer(axis, step), device_id_type=MESH)
    pl.semaphore_signal(barrier, inc=1, device_id=peer(3, 0), device_id_type=MESH)

    c_copy.wait()
    ids = lax.broadcasted_iota(jnp.int32, (experts, toks), 0)
    hot = jnp.zeros((experts, toks), jnp.float32)
    for i in range(choice_num):
        hot += jnp.where(cv[i:i + 1, :] == ids, 1.0, 0.0)
    counts = dot_nt(jnp.ones((8, toks), jnp.bfloat16), hot.astype(jnp.bfloat16))
    sbuf[0] = counts

    zs[...] = jnp.zeros_like(zs)

    def logits(j):
        a, b = load(j)
        a.wait()
        b.wait()
        cols = pl.ds(pl.multiple_of(j * LOAD_COLS, LOAD_COLS), LOAD_COLS)
        xj = xv[:, cols]
        terms = split3(part[:, cols])
        for i in range(3):
            ws[i, :, cols] = terms[i]
        zs[...] += dot_nt(xj, terms[0]) + dot_nt(xj, terms[1]) + dot_nt(xj, terms[2])

    early = min(2, nload)

    @pl.loop(0, early)
    def _(j):
        logits(j)

    pl.semaphore_wait(barrier, 10)
    for n, step in enumerate((1, 3, 2)):
        send(("s", 0, n), sbuf.at[0], srecv.at[0, n], peer(0, step))

    @pl.loop(early, nload)
    def _(j):
        logits(j)

    for n in range(3):
        arrive(("s", 0, n))
    seq_counts = (sbuf[0] + srecv[0, 2]) + (srecv[0, 0] + srecv[0, 1])
    loss_scale = ALPHA * experts / (rows_all * choice_num * seq_all * seq_all)
    weight = seq_counts[0:1, :] * loss_scale
    sig = lax.logistic(zs[...])
    total = jnp.sum(sig, axis=1, keepdims=True)
    normed = sig / total
    mixed = jnp.sum(normed * weight, axis=1, keepdims=True)
    g = (weight - mixed) * (sig * (1.0 - sig) / total)
    for i, t in enumerate(split3(g)):
        gs[i] = t
    for i, t in enumerate(split3(g.T)):
        gts[i] = t
    loss = jnp.broadcast_to(jnp.sum(mixed, axis=0, keepdims=True), (8, experts))
    is_count = lax.broadcasted_iota(jnp.int32, (8, experts), 0) < 4

    def stat_start(stage):
        sbuf[stage] = stat_val[0]
        if stage == 4:
            send(("s", 4, 0), sbuf.at[4], srecv.at[4, 0], peer(3, 0))
        else:
            for n, step in enumerate((1, 3, 2)):
                send(("s", stage, n), sbuf.at[stage], srecv.at[stage, n], peer(stage - 1, step))

    def stat_end(stage):
        if stage == 4:
            arrive(("s", 4, 0))
            new = sbuf[4] + srecv[4, 0]
        else:
            for n in range(3):
                arrive(("s", stage, n))
            new = (sbuf[stage] + srecv[stage, 2]) + (srecv[stage, 0] + srecv[stage, 1])
            if stage == 1:
                new = jnp.where(is_count, seq_counts, new)
        stat_val[0] = new

    stat_val = [loss]

    regions = make_regions(dim)
    own_e = pl.ds(pl.multiple_of(core * half_e, half_e), half_e)
    oth_e = pl.ds(pl.multiple_of(other * half_e, half_e), half_e)

    def dw_unit(u):
        cols = pl.ds(pl.multiple_of(u * UNIT, UNIT), UNIT)
        xu = xv[:, cols]
        part[:, cols] = dot_nn(gts[0], xu) + dot_nn(gts[1], xu) + dot_nn(gts[2], xu)

    def dx_unit(u):
        cols = pl.ds(pl.multiple_of(u * DX_COLS, DX_COLS), DX_COLS)
        w0, w1, w2 = ws[0, :, cols], ws[1, :, cols], ws[2, :, cols]
        g0, g1, g2 = gs[0], gs[1], gs[2]
        val = dot_nn(g2, w0) + dot_nn(g0, w2) + dot_nn(g1, w1) + dot_nn(g1, w0) + dot_nn(g0, w1) + dot_nn(g0, w0)
        dx[:, cols] = val.astype(jnp.bfloat16)

    dx_done = [0]

    def dx_some(num):
        end = min(dx_done[0] + num, dim // DX_COLS)
        if end > dx_done[0]:
            pl.loop(dx_done[0], end)(dx_unit)
        dx_done[0] = end

    def cols_of(q, h=None):
        _, _, at, wd, hf = regions[q]
        if h is None:
            return pl.ds(at, wd)
        return pl.ds(at, hf) if h == 0 else pl.ds(at + hf, wd - hf)

    def rows(start, size):
        return pl.ds(pl.multiple_of(start, 8), size)

    def axes(q):
        o = regions[q][1]
        return o, (o + 1) % 3, (o + 2) % 3

    def place(q):
        a_ax, b_ax, _ = axes(q)
        return coord[a_ax], coord[b_ax]

    def pair_start(q):
        send(("p", q), part.at[oth_e, cols_of(q)], acc.at[:, cols_of(q)], peer(3, 0))

    def pair_end(q):
        arrive(("p", q))
        acc[:, cols_of(q)] += part[own_e, cols_of(q)]

    def rs1_start(q):
        a_ax = axes(q)[0]
        a, _ = place(q)
        hp = p1 // 2
        for h, step in enumerate(STEPS):
            send(("1o", q, h), acc.at[rows(p1 * lax.rem(a + 2, RING) + hp * h, hp), cols_of(q)],
                 r1.at[0, rows(hp * h, hp), cols_of(q)], peer(a_ax, step))
        for h, step in enumerate(STEPS):
            send(("1d", q, h), acc.at[rows(p1 * lax.rem(a + step, RING) + hp * (1 - h), hp), cols_of(q)],
                 r1.at[1, rows(hp * (1 - h), hp), cols_of(q)], peer(a_ax, step))

    def rs1_mid(q):
        a_ax = axes(q)[0]
        a, _ = place(q)
        hp = p1 // 2
        for h, step in enumerate(STEPS):
            arrive(("1o", q, h))
            here = rows(p1 * lax.rem(a + step, RING) + hp * h, hp)
            acc[here, cols_of(q)] += r1[0, hp * h:hp * h + hp, cols_of(q)]
            send(("1r", q, h), acc.at[here, cols_of(q)], r1.at[2, rows(hp * h, hp), cols_of(q)], peer(a_ax, step))

    def rs1_end(q):
        a, _ = place(q)
        for h in range(2):
            arrive(("1d", q, h))
            arrive(("1r", q, h))
        acc[rows(p1 * a, p1), cols_of(q)] += r1[1, :, cols_of(q)] + r1[2, :, cols_of(q)]

    def rs2_start(q):
        b_ax = axes(q)[1]
        a, b = place(q)
        for h, step in enumerate(STEPS):
            send(("2o", q, h), acc.at[rows(p1 * a + p2 * lax.rem(b + 2, RING), p2), cols_of(q, h)],
                 r2.at[0, :, cols_of(q, h)], peer(b_ax, step))
        for h, step in enumerate(STEPS):
            send(("2d", q, h), acc.at[rows(p1 * a + p2 * lax.rem(b + step, RING), p2), cols_of(q, 1 - h)],
                 r2.at[1, :, cols_of(q, 1 - h)], peer(b_ax, step))

    def rs2_mid(q):
        b_ax = axes(q)[1]
        a, b = place(q)
        for h, step in enumerate(STEPS):
            arrive(("2o", q, h))
            here = rows(p1 * a + p2 * lax.rem(b + step, RING), p2)
            acc[here, cols_of(q, h)] += r2[0, :, cols_of(q, h)]
            send(("2r", q, h), acc.at[here, cols_of(q, h)], r2.at[2, :, cols_of(q, h)], peer(b_ax, step))

    def rs2_end(q):
        a, b = place(q)
        for h in range(2):
            arrive(("2d", q, h))
            arrive(("2r", q, h))
        here = rows(p1 * a + p2 * b, p2)
        acc[here, cols_of(q)] += r2[1, :, cols_of(q)] + r2[2, :, cols_of(q)]
        for n, step in enumerate((1, 3, 2)):
            send(("3", q, n), acc.at[here, cols_of(q)], r3.at[n, :, cols_of(q)], peer(axes(q)[2], step))

    def mine(q):
        a, b = place(q)
        return core * half_e + p1 * a + p2 * b

    def x3_end(q):
        a, b = place(q)
        for n in range(3):
            arrive(("3", q, n))
        val = (acc[rows(p1 * a + p2 * b, p2), cols_of(q)] + r3[2, :, cols_of(q)]) + (r3[0, :, cols_of(q)] + r3[1, :, cols_of(q)])
        dw[rows(mine(q), p2), cols_of(q)] = val
        for kind in range(2):
            for h, step in enumerate(STEPS):
                ref = dw.at[rows(mine(q), p2), cols_of(q, h if kind == 0 else 1 - h)]
                send(("g2", q, kind, h), ref, ref, peer(axes(q)[1], step))

    def ag2_mid(q):
        a, b = place(q)
        for h, step in enumerate(STEPS):
            arrive(("g2", q, 0, h))
            ref = dw.at[rows(core * half_e + p1 * a + p2 * lax.rem(b + (RING - step), RING), p2), cols_of(q, h)]
            send(("g2", q, 2, h), ref, ref, peer(axes(q)[1], step))

    def ag2_end(q):
        for h in range(2):
            arrive(("g2", q, 1, h))
            arrive(("g2", q, 2, h))
        a, _ = place(q)
        hp = p1 // 2
        for kind in range(2):
            for h, step in enumerate(STEPS):
                k = h if kind == 0 else 1 - h
                ref = dw.at[rows(core * half_e + p1 * a + hp * k, hp), cols_of(q)]
                send(("g1", q, kind, h), ref, ref, peer(axes(q)[0], step))
        ref = dw.at[rows(core * half_e + p1 * a, p1), cols_of(q)]
        send(("gp", q, 0), ref, ref, peer(3, 0))

    def to_partner(q, kind, h, shift, k):
        a, _ = place(q)
        hp = p1 // 2
        ref = dw.at[rows(core * half_e + p1 * lax.rem(a + shift, RING) + hp * k, hp), cols_of(q)]
        send(("gp", q, 1, kind, h), ref, ref, peer(3, 0))
        return ref

    def ag1_mid(q):
        for h, step in enumerate(STEPS):
            arrive(("g1", q, 0, h))
            a, _ = place(q)
            hp = p1 // 2
            ref = dw.at[rows(core * half_e + p1 * lax.rem(a + (RING - step), RING) + hp * h, hp), cols_of(q)]
            send(("g1", q, 2, h), ref, ref, peer(axes(q)[0], step))
            to_partner(q, 0, h, RING - step, h)

    def ag1_end(q):
        for h, step in enumerate(STEPS):
            arrive(("g1", q, 1, h))
            to_partner(q, 1, h, RING - step, 1 - h)
        for h, step in enumerate(STEPS):
            arrive(("g1", q, 2, h))
            to_partner(q, 2, h, 2, h)

    def each(chunk, f):
        for q, reg in enumerate(regions):
            if reg[0] == chunk:
                f(q)

    stat_start(1)
    unit = 0
    for q, (_, _, at, wd, _) in enumerate(regions):
        need = -(-(at + wd) // UNIT)
        pl.loop(unit, need)(dw_unit)
        unit = need
        pair_start(q)
        if q >= 1:
            pair_end(q - 1)
            rs1_start(q - 1)
    last = len(regions) - 1
    dx_some(1)
    pair_end(last)
    rs1_start(last)
    stat_end(1)
    stat_start(2)
    dx_some(1)
    each(0, rs1_mid)
    dx_some(2)
    each(1, rs1_mid)
    stat_end(2)
    stat_start(3)
    dx_some(2)
    each(0, rs1_end)
    each(0, rs2_start)
    dx_some(2)
    each(0, rs2_mid)
    each(1, rs1_end)
    each(1, rs2_start)
    stat_end(3)
    stat_start(4)
    dx_some(1)
    each(0, rs2_end)
    each(1, rs2_mid)
    dx_some(1)
    each(0, x3_end)
    each(1, rs2_end)
    dx_some(1)
    each(0, ag2_mid)
    each(0, ag2_end)
    each(1, x3_end)
    dx_some(1)
    each(1, ag2_mid)
    each(0, ag1_mid)
    each(1, ag2_end)
    stat_end(4)
    dx_some(dim)
    loads = stat_val[0][0:1, :]
    gap = rows_all * seq_all * choice_num - loads * experts
    new_bias = bias_ref[...] + GAMMA * jnp.where(gap > 0, 1.0, jnp.where(gap < 0, -1.0, 0.0))
    stat_ref[...] = jnp.where(is_count, jnp.broadcast_to(new_bias, (8, experts)), stat_val[0])
    each(0, ag1_end)
    each(1, ag1_mid)
    each(1, ag1_end)
    for key, cpy in copies.items():
        if key[0] == "gp":
            cpy.wait_recv()
    for cpy in copies.values():
        cpy.wait_send()


def num_copies():
    return 3 * 4 + 1 + CHUNKS * 3 * (1 + 6 + 6 + 3 + 6 + 6 + 7)


def solution(mesh):
    cp_size = mesh.shape["cp"]
    dp_size = mesh.shape["dp"]

    def local_step(tokens, choices, router_w, expert_bias):
        rows_all = tokens.shape[0] * dp_size
        seq_all = tokens.shape[1] * cp_size
        toks, dim = tokens.shape[1:]
        experts = router_w.shape[0]
        choice_num = choices.shape[2]
        sizes = (experts, dim, toks, choice_num, rows_all, seq_all)
        half_e = experts // 2
        nload = dim // LOAD_COLS
        n = num_copies()
        f32, bf16 = jnp.float32, jnp.bfloat16
        anyspace = pl.BlockSpec(memory_space=pl.ANY)
        vm = pl.BlockSpec(memory_space=pltpu.VMEM)
        call = pl.pallas_call(
            functools.partial(kernel, sizes),
            in_specs=[anyspace, anyspace, anyspace, vm],
            out_specs=[vm, vm, vm],
            out_shape=[pltpu.VMEM((experts, dim), f32), pltpu.VMEM((toks, dim), bf16), pltpu.VMEM((8, experts), f32)],
            scratch_shapes=[
                pltpu.VMEM((toks, dim), bf16),
                pltpu.VMEM((choice_num, toks), jnp.int32),
                pltpu.VMEM((3, experts, dim), bf16),
                pltpu.VMEM((experts, dim), f32),
                pltpu.VMEM((half_e, dim), f32),
                pltpu.VMEM((3, half_e // RING, dim), f32),
                pltpu.VMEM((3, half_e // RING // RING, dim), f32),
                pltpu.VMEM((3, half_e // RING // RING, dim), f32),
                pltpu.VMEM((toks, experts), f32),
                pltpu.VMEM((3, toks, experts), bf16),
                pltpu.VMEM((3, experts, toks), bf16),
                pltpu.VMEM((5, 8, experts), f32),
                pltpu.VMEM((5, 3, 8, experts), f32),
                pltpu.SemaphoreType.DMA((2 * nload + 1,)),
                pltpu.SemaphoreType.DMA((n,)),
                pltpu.SemaphoreType.DMA((n,)),
            ],
            compiler_params=pltpu.CompilerParams(collective_id=0, has_side_effects=True, vmem_limit_bytes=44 * 1024 * 1024),
            name="router_step",
        )
        dw, dx, stat = call(tokens[0], choices[0].T, router_w, expert_bias[None, :])
        return stat[4, 0], dw, dx[None], stat[0]

    tok_spec = P("dp", "cp", None)
    return jax.shard_map(local_step, mesh=mesh, in_specs=(tok_spec, tok_spec, P(), P()), out_specs=(P(), P(), tok_spec, P()), check_vma=False)
```
